32 devices in a mesh: chan: 2 (over x), vis: 2 (over core), pix: 8 (over z, y).
Axes of the slice: x: 2, y: 2, z: 4, core: 2. Of those that a mesh axis runs over, the one named last changes fastest.
Arguments:
- response: bfloat16 [16384, 49152], P(('chan', 'vis'), 'pix'), parts along dimension 0, may hold values from -5 to 5
- vis_data: float32 [16384], P(('chan', 'vis')), parts along dimension 0, may hold values from -6 to 6
- baseline_of_row: int32 [8192], P('vis'), may hold values from 0 to 8191
- noise_class: int32 [8192], P('vis'), may hold values from 0 to 15
- baseline_weight: float32 [8192], replicated, may hold values from 0.25 to 4
- class_inv_var: float32 [32], P('chan'), parts along dimension 0, may hold values from 0.25 to 4
Outputs:
- sky_map: float32 [98304], P(('chan', 'pix')), parts along dimension 0
- psf: float32 [98304, 64], P(('chan', 'pix'), 'vis'), parts along dimension 0
The draws below stay inside these ranges and needn't reach their ends.
There are 2 independent parts, one for each index of `chan`. The reference program is written for one: setup_inputs(seed, part) draws one part's arguments, and reference() takes and returns one part's arrays. A program takes and returns all parts, laid end to end along the dimension named above; an argument that names none is the same for every part. Nothing has to cross between parts.
Inputs may be any that keep to these rules, and one draw needn't show every extreme that they name: `baseline_of_row`: baseline index of each row.
All inputs are finite; a program needn't handle non-finite values.
Results may differ from the reference program's by a relative error of at most 0.0041.
Values may be sent and summed in bfloat16 or wider, within the bound.
A program may use at most 128 MiB of HBM per device.

```python
import math
import jax
import jax.numpy as jnp
from jax import lax

PIX = 49152
PANEL_DEV = 8
NBL = 8192
NCLASS = 16
VIS = 8192
N_PIX = 8


def with_ends(entries, stream_key, smallest, largest):
    place = [jax.random.randint(jax.random.fold_in(stream_key, axis), (), 0, length) for axis, length in enumerate(entries.shape)]
    longest = entries.shape.index(max(entries.shape))
    beside = place[:longest] + [(place[longest] + 1) % entries.shape[longest]] + place[longest + 1:]
    return entries.at[tuple(place)].set(smallest).at[tuple(beside)].set(largest)


def steps_of(own_key, dims, shards, least, top_value):
    def one(axis_at, parts):
        draws = jax.random.uniform(jax.random.fold_in(jax.random.fold_in(own_key, 6), axis_at), (parts,), jnp.float32, least / len(shards), top_value / len(shards))
        return jnp.repeat(jnp.exp(draws), dims[axis_at] // parts).reshape((-1,) + (1,) * (len(dims) - axis_at - 1))

    gain = one(*shards[0])
    for cut in shards[1:]:
        gain = gain * one(*cut)
    return gain


def noise(key, extent, spread, limit, cuts=(), held_as=jnp.bfloat16):
    loudness = steps_of(key, extent, cuts, -0.22, 0.18) if cuts else 1.0
    result = jax.random.normal(key, extent, jnp.float32) * spread * loudness
    return jnp.minimum(jnp.maximum(result, -limit), limit).astype(held_as)


def setup_inputs(seed: int = 0, part: int = 0) -> dict:
    seeds = jax.random.split(jax.random.key(seed), 7)
    part_keys = jax.random.split(jax.random.fold_in(seeds[6], part), 7)
    return {
        "response": noise(part_keys[0], (VIS, PIX), 1.0, 5.0, ((0, 2), (1, 8))),
        "vis_data": noise(part_keys[1], (VIS,), 1.0, 6.0, ((0, 2),), jnp.float32),
        "baseline_of_row": with_ends(jax.random.randint(seeds[2], (VIS,), 0, NBL), jax.random.fold_in(seeds[2], 1), 0, NBL - 1).astype(jnp.int32),
        "noise_class": with_ends(jax.random.randint(seeds[3], (VIS,), 0, NCLASS), jax.random.fold_in(seeds[3], 1), 0, NCLASS - 1).astype(jnp.int32),
        "baseline_weight": jnp.clip(jnp.exp(jax.random.uniform(seeds[4], (NBL,), jnp.float32, math.log(0.25), math.log(4.0))), 0.25, 4.0),
        "class_inv_var": jnp.clip(jnp.exp(jax.random.uniform(part_keys[5], (NCLASS,), jnp.float32, math.log(0.25), math.log(4.0))), 0.25, 4.0),
    }


def add_norm(total, pair):
    resp_block, weight_block = pair
    squares = jnp.square(resp_block.astype(jnp.float32))
    return (total + lax.optimization_barrier(jnp.sum(weight_block[:, None] * squares, axis=0)), None)

def reference(response, vis_data, baseline_of_row, noise_class, baseline_weight, class_inv_var):
    weight_row = baseline_weight[baseline_of_row] * class_inv_var[noise_class]
    pix_block = PIX // N_PIX
    blocks = response.reshape(VIS, N_PIX, pix_block)
    panel_cols = blocks[:, :, :PANEL_DEV].reshape(VIS, N_PIX * PANEL_DEV)
    weighted_panel = (weight_row[:, None] * panel_cols.astype(jnp.float32)).astype(jnp.bfloat16)
    weighted_vis = (weight_row * vis_data).astype(jnp.bfloat16)
    dirty_map = jnp.dot(weighted_vis, response, preferred_element_type=jnp.float32)
    row_step = math.gcd(VIS, 512)
    stacked = response.reshape(VIS // row_step, row_step, PIX)
    stacked_weight = weight_row.reshape(VIS // row_step, row_step)
    pixel_norm, unused = lax.scan(add_norm, jnp.zeros((PIX,), jnp.float32), (stacked, stacked_weight))
    beam_full = jnp.dot(response.T, weighted_panel, preferred_element_type=jnp.float32)
    panel_norm = pixel_norm.reshape(N_PIX, pix_block)[:, :PANEL_DEV].reshape(N_PIX * PANEL_DEV)
    sky_map = dirty_map / jnp.sqrt(pixel_norm)
    psf = beam_full / jnp.sqrt(pixel_norm[:, None] * panel_norm[None, :])
    return (sky_map, psf)
```

```python
import functools

import jax
import jax.numpy as jnp
from jax import lax
from jax.experimental import pallas as pl
from jax.experimental.pallas import tpu as pltpu
from jax.sharding import PartitionSpec as P

PANEL_DEV = 8
LANES = 128
TILE = 256
EXTRA = 16
MESH_ID = pl.DeviceIdType.MESH
F32, BF16 = jnp.float32, jnp.bfloat16


def kernel(
    n_pix, n_in, n_block, ch,
    resp, vis_h, base_h, cls_h, bw_h, civ_h,
    sky, psf,
    x, vis, base, cls, bw, civ, pbuf, w_ref, wcol, lhs, nacc, acc, rbuf,
    qbuf, qown, qrecv,
    in_sem, small_sem, psend, precv, vsend, vrecv, qsem,
):
    rows, pix = x.shape
    rb = rows // n_block
    n_panel = n_pix * PANEL_DEV
    half = n_panel // 2
    me = lax.axis_index("pix")
    v = lax.axis_index("vis")
    other = 1 - v
    n_out = n_pix // n_in
    zi, yi = me // n_in, lax.rem(me, n_in)

    def slot_of(source):
        return lax.rem(source + v * (n_pix // 2), n_pix)

    def line(d):
        return lax.rem(zi + d, n_out) * n_in + yi

    def side(d):
        return zi * n_in + lax.rem(yi + d, n_in)

    home = slot_of(me)

    smalls = [
        pltpu.make_async_copy(a, b, small_sem.at[i])
        for i, (a, b) in enumerate(
            [(base_h, base), (bw_h, bw), (cls_h, cls), (civ_h, civ), (vis_h, vis)]
        )
    ]
    for c in smalls:
        c.start()
    first = pltpu.make_async_copy(
        resp.at[:, pl.ds(0, LANES)], x.at[:, pl.ds(0, LANES)], small_sem.at[5]
    )
    first.start()

    def piece(r, c):
        lo = LANES if c == 0 else c * ch
        at = (pl.ds(r * rb, rb), pl.ds(lo, (c + 1) * ch - lo))
        return pltpu.make_async_copy(resp.at[at], x.at[at], in_sem.at[r, c])

    def has_piece(c):
        return ch > LANES or c > 0

    for r in range(n_block):
        for c in range(pix // ch):
            if has_piece(c):
                piece(r, c).start(priority=1)

    barrier = pltpu.get_barrier_semaphore()

    for d in range(1, n_out):
        pl.semaphore_signal(
            barrier, inc=1, device_id={"pix": line(d)}, device_id_type=MESH_ID
        )
    for d in range(1, n_in):
        pl.semaphore_signal(
            barrier, inc=1, device_id={"pix": side(d)}, device_id_type=MESH_ID
        )
    pl.semaphore_signal(barrier, inc=1, device_id={"vis": other}, device_id_type=MESH_ID)

    for c in smalls:
        c.wait()
    n_hi = bw.shape[0]
    t0 = bw[...].astype(BF16)
    left = bw[...] - t0.astype(F32)
    t1 = left.astype(BF16)
    t2 = (left - t1.astype(F32)).astype(BF16)
    table = jnp.concatenate([t0, t1, t2], axis=0)
    n_cls = civ.shape[1]
    diag = lax.broadcasted_iota(jnp.int32, (n_cls, n_cls), 0) == lax.broadcasted_iota(
        jnp.int32, (n_cls, n_cls), 1
    )
    civ_col = jnp.sum(
        jnp.where(diag, jnp.broadcast_to(civ[...], (n_cls, n_cls)), 0.0), axis=1, keepdims=True
    )
    step = min(rows, 512)
    with jax.named_scope("weights"):
        for i in range(rows // step):
            cols = pl.ds(i * step, step)
            idx = base[:, cols]
            hi = lax.broadcast_in_dim(idx // LANES, (n_hi, step), (0, 1))
            lo = lax.broadcast_in_dim(lax.rem(idx, LANES), (LANES, step), (0, 1))
            hot = (hi == lax.broadcasted_iota(jnp.int32, (n_hi, step), 0)).astype(F32).astype(BF16)
            picked = lax.dot_general(
                table, jnp.concatenate([hot] * 3, axis=0), (((0,), (0,)), ((), ())),
                preferred_element_type=F32,
            )
            bw_row = jnp.sum(
                jnp.where(lo == lax.broadcasted_iota(jnp.int32, (LANES, step), 0), picked, 0.0),
                axis=0, keepdims=True,
            )
            kinds = lax.broadcast_in_dim(cls[:, cols], (n_cls, step), (0, 1))
            cw_row = jnp.sum(
                jnp.where(
                    kinds == lax.broadcasted_iota(jnp.int32, (n_cls, step), 0), civ_col, 0.0
                ),
                axis=0, keepdims=True,
            )
            w_ref[:, cols] = jnp.broadcast_to(bw_row * cw_row, (PANEL_DEV, step))

    with jax.named_scope("panel"):
        first.wait()
        pick = (
            lax.broadcasted_iota(jnp.int32, (16, LANES), 0)
            == lax.broadcasted_iota(jnp.int32, (16, LANES), 1)
        ).astype(BF16)
        sums = jnp.zeros((PANEL_DEV, 1), F32)
        for r in range(n_block):
            at = pl.ds(r * rb, rb)
            own = lax.dot_general(
                pick, x[at, :LANES], (((1,), (1,)), ((), ())), preferred_element_type=F32
            )[:PANEL_DEV]
            weighted = own * w_ref[:, at]
            sums = sums + jnp.sum(weighted * own, axis=1, keepdims=True)
            pbuf[r, home] = weighted.astype(BF16)
        qbuf[home] = jnp.broadcast_to(sums, (PANEL_DEV, LANES))

    with jax.named_scope("barrier"):
        pl.semaphore_wait(barrier, n_out + n_in - 1)

    def panel_copy(r, source, peer, i):
        slot = slot_of(source)
        if r == n_block:
            return pltpu.make_async_remote_copy(
                src_ref=qbuf.at[slot], dst_ref=qbuf.at[slot],
                send_sem=psend.at[r, i], recv_sem=precv.at[r, slot],
                device_id={"pix": peer}, device_id_type=MESH_ID,
            )
        return pltpu.make_async_remote_copy(
            src_ref=pbuf.at[r, slot], dst_ref=pbuf.at[r, slot],
            send_sem=psend.at[r, i], recv_sem=precv.at[r, slot],
            device_id={"pix": peer}, device_id_type=MESH_ID,
        )

    def own_copies(r):
        out = [panel_copy(r, me, line(d), d - 1) for d in range(n_out - 1, 0, -1)]
        return out + [panel_copy(r, me, side(d), n_out + d - 2) for d in range(1, n_in)]

    def relay(r, d, e):
        return panel_copy(r, line(d), side(e), n_out + n_in - 2 + (d - 1) * (n_in - 1) + e - 1)

    for r in range(n_block + 1):
        for c in own_copies(r):
            c.start()

    def forward(r):
        with jax.named_scope("forward%d" % r):
            for d in range(1, n_out):
                panel_copy(r, line(d), me, 0).wait_recv()
                for e in range(1, n_in):
                    relay(r, d, e).start()

    with jax.named_scope("wcol"):
        at = lax.broadcasted_iota(jnp.int32, (EXTRA, rb), 0)
        unit = (lax.broadcasted_iota(jnp.int32, (EXTRA, LANES), 0) == 0).astype(BF16)
        for r in range(n_block):
            cols = pl.ds(r * rb, rb)
            w = jnp.concatenate([w_ref[:, cols]] * 2, axis=0)
            lhs[n_panel : n_panel + EXTRA, cols] = jnp.where(at == 0, w * vis[:, cols], 0.0).astype(BF16)
            wcol[cols, :] = lax.dot_general(
                w.astype(BF16), unit, (((0,), (0,)), ((), ())), preferred_element_type=F32
            ).astype(BF16)

    fold = rb // TILE if rb % TILE == 0 else 1
    kb = rb // fold
    ones = jnp.ones((16, kb), BF16)
    pad = lhs.shape[0] - n_panel - EXTRA
    if pad:
        lhs[n_panel + EXTRA :, :] = jnp.zeros((pad, rows), BF16)

    def norm_part(r, lo, n):
        parts = []
        wide = TILE if n % TILE == 0 else LANES
        for s in range(lo, lo + n, wide):
            total = None
            for i in range(fold):
                at = pl.ds(r * rb + i * kb, kb)
                xb = x[at, pl.ds(s, wide)]
                term = xb * xb * jnp.concatenate([wcol[at, :]] * (wide // LANES), axis=1)
                total = term if total is None else total + term
            parts.append(jnp.dot(ones, total, preferred_element_type=F32)[:8])
        return jnp.concatenate(parts, axis=1) if len(parts) > 1 else parts[0]

    def norm_step(r, c):
        wait_x(r, c)
        cols = pl.ds(c * ch, ch)
        got = norm_part(r, c * ch, ch)
        nacc[:, cols] = got if r == 0 else nacc[:, cols] + got

    def beam_part(r, lo, n):
        cols = pl.ds(lo, n)
        return jnp.dot(
            lhs[:, r * rb : (r + 1) * rb], x[r * rb : (r + 1) * rb, cols],
            preferred_element_type=F32,
        )[: n_panel + 8]

    sub = next(s for s in (512, 384, 256, 128) if ch % s == 0)

    def beam_step(r, c):
        for lo in range(c * ch, (c + 1) * ch, sub):
            got = beam_part(r, lo, sub)
            cols = pl.ds(lo, sub)
            acc[:, cols] = got if r == 0 else acc[:, cols] + got

    def wait_x(r, c):
        if has_piece(c):
            piece(r, c).wait()

    def others(r):
        def one(i, carry):
            d, e = i // (n_in - 1), lax.rem(i, n_in - 1) + 1
            source = lax.rem(zi + d, n_out) * n_in + lax.rem(yi + e, n_in)
            panel_copy(r, source, me, 0).wait_recv()
            return carry

        lax.fori_loop(0, n_out * (n_in - 1), one, 0)

    def panel(r):
        with jax.named_scope("panel%d" % r):
            others(r)
            cols = pl.ds(r * rb, rb)
            for j in range(n_pix // 2):
                lhs[16 * j : 16 * j + 16, cols] = jnp.concatenate(
                    [pbuf[r, 2 * j], pbuf[r, 2 * j + 1]], axis=0
                )

    wide = pix // ch
    last = n_block - 1
    todo = []
    if n_block == 4:
        todo += [("A", 0, c) for c in range(wide)]
        todo += [("A", 1, c) for c in range(wide - 1)] + [("F", 0, 0)]
        todo += [("A", 1, wide - 1), ("F", 1, 0), ("A", 2, 0), ("F", 2, 0)]
        todo += [("A", 2, c) for c in range(1, wide)]
        todo += [("P", 0, 0)] + [("B", 0, c) for c in range(wide)]
        todo += [("F", 3, 0), ("F", 4, 0), ("P", 1, 0), ("A", 3, 0)] + [("B", 1, c) for c in range(wide)]
        todo += [("P", 2, 0)] + [("A", 3, c) for c in range(1, wide)] + [("B", 2, c) for c in range(wide)]
    else:
        for r in range(n_block):
            todo += [("A", r, c) for c in range(wide)]
        todo += [("F", r, 0) for r in range(n_block + 1)]
        for r in range(last):
            todo += [("P", r, 0)] + [("B", r, c) for c in range(wide)]
    for kind, r, c in todo:
        if kind == "F":
            forward(r)
        elif kind == "P":
            panel(r)
        else:
            with jax.named_scope("%s%d_%d" % (kind, r, c)):
                {"A": norm_step, "B": beam_step}[kind](r, c)
    panel(last)

    with jax.named_scope("qwait"):
        others(n_block)
    q_copy = pltpu.make_async_remote_copy(
        src_ref=qbuf.at[pl.ds(n_pix // 2, n_pix // 2)], dst_ref=qrecv,
        send_sem=qsem.at[0], recv_sem=qsem.at[1],
        device_id={"vis": other}, device_id_type=MESH_ID,
    )
    q_copy.start()

    spans = [(c * ch, ch) for c in range(wide)]
    while len(spans) < wide + 2 and spans[-1][1] % (2 * sub) == 0:
        lo, n = spans.pop()
        spans += [(lo, n // 2), (lo + n // 2, n // 2)]

    def vis_copy(i):
        cols = pl.ds(*spans[i])
        return pltpu.make_async_remote_copy(
            src_ref=acc.at[pl.ds(half, half + 8), cols], dst_ref=rbuf.at[:, cols],
            send_sem=vsend.at[i], recv_sem=vrecv.at[i],
            device_id={"vis": other}, device_id_type=MESH_ID,
        )

    def last_step(i):
        for lo in range(spans[i][0], sum(spans[i]), sub):
            cols = pl.ds(lo, sub)
            got = beam_part(last, lo, sub)
            if last > 0:
                got = got + acc[:, cols]
            at = lax.broadcasted_iota(jnp.int32, (8, sub), 0)
            acc[:n_panel, cols] = got[:n_panel]
            acc[n_panel:, cols] = jnp.where(at == 1, nacc[:, cols], got[n_panel:])
        vis_copy(i).start()

    def final(i):
        vis_copy(i).wait_recv()
        for lo in range(spans[i][0], sum(spans[i]), sub):
            cols = pl.ds(lo, sub)
            pair = acc[n_panel:, cols] + rbuf[half:, cols]
            scale = lax.rsqrt(pair[1:2])
            sky[:, cols] = pair[0:1] * scale
            psf[:, cols] = (acc[:half, cols] + rbuf[:half, cols]) * scale * qown[:, :1]

    lag = 2
    for i in range(len(spans) + lag):
        if i < len(spans):
            with jax.named_scope("L%d" % i):
                last_step(i)
        if i == lag:
            with jax.named_scope("qcopy"):
                q_copy.wait()
                mine = qbuf[: n_pix // 2].reshape(half, LANES)
                qown[...] = lax.rsqrt(mine + qrecv[...].reshape(half, LANES))
        if 0 <= i - lag < len(spans):
            with jax.named_scope("final%d" % (i - lag)):
                final(i - lag)

    for i in range(len(spans)):
        vis_copy(i).wait_send()
    for r in range(n_block + 1):
        for c in own_copies(r):
            c.wait_send()
        for d in range(1, n_out):
            for e in range(1, n_in):
                relay(r, d, e).wait_send()


def shards(n_pix, response, vis_data, baseline_of_row, noise_class, baseline_weight, class_inv_var):
    rows, pix = response.shape
    ch = next(c for c in (2048, 1536, 1024, 768, 512, 384, 256, 128) if pix % c == 0)
    n_in = max(d for d in range(1, n_pix + 1) if n_pix % d == 0 and d * d <= n_pix)
    n_block = next(b for b in (4, 2, 1) if rows % (b * 256) == 0 or b == 1)
    n_panel = n_pix * PANEL_DEV
    half = n_panel // 2
    n_hi = baseline_weight.shape[0] // LANES
    n_cls = class_inv_var.shape[0]
    vmem, dma = pltpu.VMEM, pltpu.SemaphoreType.DMA
    sky, psf = pl.pallas_call(
        functools.partial(kernel, n_pix, n_in, n_block, ch),
        out_shape=(
            pltpu.VMEM((1, pix), F32),
            pltpu.VMEM((half, pix), F32),
        ),
        in_specs=[pl.BlockSpec(memory_space=pltpu.HBM)] * 6,
        out_specs=(pl.BlockSpec(memory_space=pltpu.VMEM),) * 2,
        scratch_shapes=[
            vmem((rows, pix), BF16),
            vmem((1, rows), F32),
            vmem((1, rows), jnp.int32),
            vmem((1, rows), jnp.int32),
            vmem((n_hi, LANES), F32),
            vmem((1, n_cls), F32),
            vmem((n_block, n_pix, PANEL_DEV, rows // n_block), BF16),
            vmem((PANEL_DEV, rows), F32),
            vmem((rows, LANES), BF16),
            vmem((max(n_panel + EXTRA, LANES), rows), BF16),
            vmem((8, pix), F32),
            vmem((n_panel + 8, pix), F32),
            vmem((half + 8, pix), F32),
            vmem((n_pix, PANEL_DEV, LANES), F32),
            vmem((half, LANES), F32),
            vmem((n_pix // 2, PANEL_DEV, LANES), F32),
            dma((n_block, pix // ch)),
            dma((6,)),
            dma((n_block + 1, 2 * n_pix)),
            dma((n_block + 1, n_pix)),
            dma((pix // ch + 2,)),
            dma((pix // ch + 2,)),
            dma((2,)),
        ],
        compiler_params=pltpu.CompilerParams(
            collective_id=0, has_side_effects=True, vmem_limit_bytes=60 * 1024 * 1024
        ),
    )(
        response,
        vis_data.reshape(1, rows),
        baseline_of_row.reshape(1, rows),
        noise_class.reshape(1, rows),
        baseline_weight.reshape(n_hi, LANES),
        class_inv_var.reshape(1, n_cls),
    )
    return sky.reshape(pix), psf.T


def solution(mesh):
    placed = (P(("chan", "vis"), "pix"), P(("chan", "vis")), P("vis"), P("vis"), P(), P("chan"))
    return jax.shard_map(
        functools.partial(shards, mesh.shape["pix"]),
        mesh=mesh,
        in_specs=placed,
        out_specs=(P(("chan", "pix")), P(("chan", "pix"), "vis")),
        check_vma=False,
    )
```

```python
import functools

import jax
import jax.numpy as jnp
from jax import lax
from jax.experimental import pallas as pl
from jax.experimental.pallas import tpu as pltpu
from jax.sharding import PartitionSpec as P

PANEL_DEV = 8
LANES = 128
TILE = 256
EXTRA = 16
MESH_ID = pl.DeviceIdType.MESH
F32, BF16 = jnp.float32, jnp.bfloat16


def kernel(
    n_pix, n_in, n_block, ch,
    resp, vis_h, base_h, cls_h, bw_h, civ_h,
    sky, psf,
    x, vis, base, cls, bw, civ, pbuf, w_ref, wcol, ybuf, lhs, nacc, acc, rbuf,
    qbuf, qown, qrecv,
    in_sem, small_sem, psend, precv, vsend, vrecv, qsem,
):
    rows, pix = x.shape
    rb = rows // n_block
    n_panel = n_pix * PANEL_DEV
    half = n_panel // 2
    me = lax.axis_index("pix")
    v = lax.axis_index("vis")
    other = 1 - v
    n_out = n_pix // n_in
    zi, yi = me // n_in, lax.rem(me, n_in)

    def slot_of(source):
        return lax.rem(source + v * (n_pix // 2), n_pix)

    def line(d):
        return lax.rem(zi + d, n_out) * n_in + yi

    def side(d):
        return zi * n_in + lax.rem(yi + d, n_in)

    home = slot_of(me)

    smalls = [
        pltpu.make_async_copy(a, b, small_sem.at[i])
        for i, (a, b) in enumerate(
            [(base_h, base), (bw_h, bw), (cls_h, cls), (civ_h, civ), (vis_h, vis)]
        )
    ]
    for c in smalls:
        c.start()
    first = pltpu.make_async_copy(
        resp.at[:, pl.ds(0, LANES)], x.at[:, pl.ds(0, LANES)], small_sem.at[5]
    )
    first.start()

    def piece(r, c):
        lo = LANES if c == 0 else c * ch
        at = (pl.ds(r * rb, rb), pl.ds(lo, (c + 1) * ch - lo))
        return pltpu.make_async_copy(resp.at[at], x.at[at], in_sem.at[r, c])

    def has_piece(c):
        return ch > LANES or c > 0

    for r in range(n_block):
        for c in range(pix // ch):
            if has_piece(c):
                piece(r, c).start(priority=1)

    barrier = pltpu.get_barrier_semaphore()

    for d in range(1, n_out):
        pl.semaphore_signal(
            barrier, inc=1, device_id={"pix": line(d)}, device_id_type=MESH_ID
        )
    for d in range(1, n_in):
        pl.semaphore_signal(
            barrier, inc=1, device_id={"pix": side(d)}, device_id_type=MESH_ID
        )
    pl.semaphore_signal(barrier, inc=1, device_id={"vis": other}, device_id_type=MESH_ID)

    for c in smalls:
        c.wait()
    n_hi = bw.shape[0]
    t0 = bw[...].astype(BF16)
    left = bw[...] - t0.astype(F32)
    t1 = left.astype(BF16)
    t2 = (left - t1.astype(F32)).astype(BF16)
    table = jnp.concatenate([t0, t1, t2], axis=0)
    n_cls = civ.shape[1]
    diag = lax.broadcasted_iota(jnp.int32, (n_cls, n_cls), 0) == lax.broadcasted_iota(
        jnp.int32, (n_cls, n_cls), 1
    )
    civ_col = jnp.sum(
        jnp.where(diag, jnp.broadcast_to(civ[...], (n_cls, n_cls)), 0.0), axis=1, keepdims=True
    )
    step = min(rows, 512)
    with jax.named_scope("weights"):
        for i in range(rows // step):
            cols = pl.ds(i * step, step)
            idx = base[:, cols]
            hi = lax.broadcast_in_dim(idx // LANES, (n_hi, step), (0, 1))
            lo = lax.broadcast_in_dim(lax.rem(idx, LANES), (LANES, step), (0, 1))
            hot = (hi == lax.broadcasted_iota(jnp.int32, (n_hi, step), 0)).astype(F32).astype(BF16)
            picked = lax.dot_general(
                table, jnp.concatenate([hot] * 3, axis=0), (((0,), (0,)), ((), ())),
                preferred_element_type=F32,
            )
            bw_row = jnp.sum(
                jnp.where(lo == lax.broadcasted_iota(jnp.int32, (LANES, step), 0), picked, 0.0),
                axis=0, keepdims=True,
            )
            kinds = lax.broadcast_in_dim(cls[:, cols], (n_cls, step), (0, 1))
            cw_row = jnp.sum(
                jnp.where(
                    kinds == lax.broadcasted_iota(jnp.int32, (n_cls, step), 0), civ_col, 0.0
                ),
                axis=0, keepdims=True,
            )
            w_ref[:, cols] = jnp.broadcast_to(bw_row * cw_row, (PANEL_DEV, step))

    with jax.named_scope("panel"):
        first.wait()
        pick = (
            lax.broadcasted_iota(jnp.int32, (16, LANES), 0)
            == lax.broadcasted_iota(jnp.int32, (16, LANES), 1)
        ).astype(BF16)
        sums = jnp.zeros((PANEL_DEV, 1), F32)
        for r in range(n_block):
            at = pl.ds(r * rb, rb)
            own = lax.dot_general(
                pick, x[at, :LANES], (((1,), (1,)), ((), ())), preferred_element_type=F32
            )[:PANEL_DEV]
            weighted = own * w_ref[:, at]
            sums = sums + jnp.sum(weighted * own, axis=1, keepdims=True)
            pbuf[r, home] = weighted.astype(BF16)
        qbuf[home] = jnp.broadcast_to(sums, (PANEL_DEV, LANES))

    with jax.named_scope("barrier"):
        pl.semaphore_wait(barrier, n_out + n_in - 1)

    def panel_copy(r, slot, peer, group):
        return pltpu.make_async_remote_copy(
            src_ref=pbuf.at[r, slot], dst_ref=pbuf.at[r, slot],
            send_sem=psend.at[0], recv_sem=precv.at[0 if isinstance(r, pl.Slice) else r, group],
            device_id={"pix": peer}, device_id_type=MESH_ID,
        )

    def norm_copy(slot, peer, group):
        return pltpu.make_async_remote_copy(
            src_ref=qbuf.at[slot], dst_ref=qbuf.at[slot],
            send_sem=psend.at[1], recv_sem=precv.at[n_block, group],
            device_id={"pix": peer}, device_id_type=MESH_ID,
        )

    def some_copy(r, slot, peer, group):
        return norm_copy(slot, peer, group) if r == n_block else panel_copy(r, slot, peer, group)

    def arrived(r, n, group):
        some_copy(r, pl.ds(0, n), me, group).wait_recv()

    for r in range(n_block):
        for e in range(1, n_in):
            panel_copy(r, home, side(e), 1).start()

    def send_down(i, carry):
        z, r = i // n_block, lax.rem(i, n_block)
        panel_copy(r, home, z * n_in + yi, 0).start()
        return carry

    lax.fori_loop(0, zi * n_block, send_down, 0)
    for r in range(n_block):
        def send_up(i, carry, r=r):
            panel_copy(r, home, (n_out - 1 - i) * n_in + yi, 0).start()
            return carry

        lax.fori_loop(0, n_out - 1 - zi, send_up, 0)
    for e in range(1, n_in):
        norm_copy(home, side(e), 1).start()
    for d in range(1, n_out):
        norm_copy(home, line(d), 0).start()

    def forward(r):
        with jax.named_scope("forward%d" % r):
            arrived(r, n_out - 1, 0)
            for d in range(1, n_out):
                for e in range(1, n_in):
                    some_copy(r, slot_of(line(d)), side(e), 1).start()

    with jax.named_scope("wcol"):
        at = lax.broadcasted_iota(jnp.int32, (EXTRA, rb), 0)
        unit = (lax.broadcasted_iota(jnp.int32, (EXTRA, LANES), 0) == 0).astype(BF16)
        for r in range(n_block):
            cols = pl.ds(r * rb, rb)
            w = jnp.concatenate([w_ref[:, cols]] * 2, axis=0)
            lhs[n_panel : n_panel + EXTRA, cols] = jnp.where(at == 0, w * vis[:, cols], 0.0).astype(BF16)
            wcol[cols, :] = lax.dot_general(
                w.astype(BF16), unit, (((0,), (0,)), ((), ())), preferred_element_type=F32
            ).astype(BF16)

    fold = rb // TILE if rb % TILE == 0 else 1
    kb = rb // fold
    ones = jnp.ones((16, kb), BF16)
    sub = next(s for s in (512, 384, 256, 128) if ch % s == 0)
    pad = lhs.shape[0] - n_panel - EXTRA
    if pad:
        lhs[n_panel + EXTRA :, :] = jnp.zeros((pad, rows), BF16)

    wide_t = TILE if ch % TILE == 0 else LANES
    strip = min(kb, 64)

    def fold_part(r, lo, n):
        for k in range(0, kb, strip):
            rows_of = [pl.ds(r * rb + i * kb + k, strip) for i in range(fold)]
            ws = [jnp.concatenate([wcol[at, :]] * (wide_t // LANES), axis=1) for at in rows_of]
            for s in range(0, n, wide_t):
                total = None
                for at, w in zip(rows_of, ws):
                    xb = x[at, pl.ds(lo + s, wide_t)]
                    term = xb * xb * w
                    total = term if total is None else total + term
                ybuf[k : k + strip, pl.ds(lo % ch + s, wide_t)] = total

    def norm_dot(r, c):
        for s in range(0, ch, sub):
            cols = pl.ds(c * ch + s, sub)
            got = jnp.dot(ones, ybuf[:, s : s + sub], preferred_element_type=F32)[:8]
            nacc[:, cols] = got if r == 0 else nacc[:, cols] + got

    def norm_step(r, c):
        wait_x(r, c)
        fold_part(r, c * ch, ch)
        norm_dot(r, c)

    def both_step(ra, ca, rb_, cb):
        wait_x(ra, ca)
        for s in range(0, ch, sub):
            cols = pl.ds(cb * ch + s, sub)
            got = beam_part(rb_, cb * ch + s, sub)
            acc[:, cols] = got if rb_ == 0 else acc[:, cols] + got
            fold_part(ra, ca * ch + s, sub)
        norm_dot(ra, ca)

    def beam_part(r, lo, n):
        cols = pl.ds(lo, n)
        return jnp.dot(
            lhs[:, r * rb : (r + 1) * rb], x[r * rb : (r + 1) * rb, cols],
            preferred_element_type=F32,
        )[: n_panel + 8]

    def beam_step(r, c):
        for lo in range(c * ch, (c + 1) * ch, sub):
            got = beam_part(r, lo, sub)
            cols = pl.ds(lo, sub)
            acc[:, cols] = got if r == 0 else acc[:, cols] + got

    def wait_x(r, c):
        if has_piece(c):
            piece(r, c).wait()

    def others(r):
        arrived(r, n_out * (n_in - 1), 1)

    def panel(r):
        with jax.named_scope("panel%d" % r):
            others(r)
            cols = pl.ds(r * rb, rb)
            for j in range(n_pix // 2):
                lhs[16 * j : 16 * j + 16, cols] = jnp.concatenate(
                    [pbuf[r, 2 * j], pbuf[r, 2 * j + 1]], axis=0
                )

    wide = pix // ch
    last = n_block - 1
    todo = []
    span = range(wide)
    if n_block == 4 and wide == 3:
        todo += [("A", 0, c) for c in span]
        todo += [("A", 1, 0), ("A", 1, 1), ("F", 0), ("A", 1, 2), ("F", 1), ("A", 2, 0), ("F", 2)]
        todo += [("A", 2, 1), ("F", 3), ("A", 2, 2), ("F", 4), ("P", 0), ("B", 0, 0)]
        todo += [("AB", 3, 0, 0, 1), ("B", 0, 2)]
        todo += [("P", 1), ("AB", 3, 1, 1, 0), ("B", 1, 1), ("AB", 3, 2, 1, 2)]
        todo += [("P", 2), ("B", 2, 0), ("B", 2, 1), ("B", 2, 2)]
    else:
        for r in range(n_block):
            todo += [("A", r, c) for c in span]
        todo += [("F", r) for r in range(n_block + 1)]
        for r in range(last):
            todo += [("P", r)] + [("B", r, c) for c in span]
    run = {"A": norm_step, "B": beam_step, "AB": both_step, "F": forward, "P": panel}
    for kind, *where in todo:
        with jax.named_scope("%s%s" % (kind, "_".join(map(str, where)))):
            run[kind](*where)
    panel(last)

    with jax.named_scope("qwait"):
        others(n_block)
    q_copy = pltpu.make_async_remote_copy(
        src_ref=qbuf.at[pl.ds(n_pix // 2, n_pix // 2)], dst_ref=qrecv,
        send_sem=qsem.at[0], recv_sem=qsem.at[1],
        device_id={"vis": other}, device_id_type=MESH_ID,
    )
    q_copy.start()

    spans = [(c * ch, ch) for c in range(wide)]
    while len(spans) < wide + 2 and spans[-1][1] % (2 * sub) == 0:
        lo, n = spans.pop()
        spans += [(lo, n // 2), (lo + n // 2, n // 2)]

    def vis_copy(i):
        cols = pl.ds(*spans[i])
        return pltpu.make_async_remote_copy(
            src_ref=acc.at[pl.ds(half, half + 8), cols], dst_ref=rbuf.at[:, cols],
            send_sem=vsend.at[0], recv_sem=vrecv.at[i],
            device_id={"vis": other}, device_id_type=MESH_ID,
        )

    def last_step(i):
        for lo in range(spans[i][0], sum(spans[i]), sub):
            cols = pl.ds(lo, sub)
            got = beam_part(last, lo, sub)
            if last > 0:
                got = got + acc[:, cols]
            at = lax.broadcasted_iota(jnp.int32, (8, sub), 0)
            acc[:n_panel, cols] = got[:n_panel]
            acc[n_panel:, cols] = jnp.where(at == 1, nacc[:, cols], got[n_panel:])
        vis_copy(i).start()

    def final(i):
        vis_copy(i).wait_recv()
        for lo in range(spans[i][0], sum(spans[i]), sub):
            cols = pl.ds(lo, sub)
            pair = acc[n_panel:, cols] + rbuf[half:, cols]
            scale = lax.rsqrt(pair[1:2])
            sky[:, cols] = pair[0:1] * scale
            psf[:, cols] = (acc[:half, cols] + rbuf[:half, cols]) * scale * qown[:, :1]

    lag = len(spans)
    for i in range(len(spans) + lag):
        if i < len(spans):
            with jax.named_scope("L%d" % i):
                last_step(i)
        if i == lag:
            with jax.named_scope("qcopy"):
                q_copy.wait()
                mine = qbuf[: n_pix // 2].reshape(half, LANES)
                qown[...] = lax.rsqrt(mine + qrecv[...].reshape(half, LANES))
        if 0 <= i - lag < len(spans):
            with jax.named_scope("final%d" % (i - lag)):
                final(i - lag)

    pltpu.make_async_remote_copy(
        src_ref=acc.at[pl.ds(half, half + 8), :], dst_ref=rbuf,
        send_sem=vsend.at[0], recv_sem=vrecv.at[0],
        device_id={"vis": other}, device_id_type=MESH_ID,
    ).wait_send()
    panel_copy(pl.ds(0, n_block), pl.ds(0, n_pix - 1), me, 0).wait_send()
    norm_copy(pl.ds(0, n_pix - 1), me, 0).wait_send()


def flush(sky, psf, sky_h, psf_h, sem):
    copies = [
        pltpu.make_async_copy(a, b, sem.at[i])
        for i, (a, b) in enumerate([(psf, psf_h), (sky, sky_h)])
    ]
    for c in copies:
        c.start()
    for c in copies:
        c.wait()


def shards(n_pix, response, vis_data, baseline_of_row, noise_class, baseline_weight, class_inv_var):
    rows, pix = response.shape
    ch = next(c for c in (2048, 1536, 1024, 768, 512, 384, 256, 128) if pix % c == 0)
    n_in = max(d for d in range(1, n_pix + 1) if n_pix % d == 0 and d * d <= n_pix)
    n_block = next(b for b in (4, 2, 1) if rows % (b * 256) == 0 or b == 1)
    n_panel = n_pix * PANEL_DEV
    half = n_panel // 2
    n_hi = baseline_weight.shape[0] // LANES
    n_cls = class_inv_var.shape[0]
    vmem, dma = pltpu.VMEM, pltpu.SemaphoreType.DMA
    sky, psf = pl.pallas_call(
        functools.partial(kernel, n_pix, n_in, n_block, ch),
        out_shape=(
            pltpu.VMEM((1, pix), F32),
            pltpu.VMEM((half, pix), F32),
        ),
        in_specs=[pl.BlockSpec(memory_space=pltpu.HBM)] * 6,
        out_specs=(pl.BlockSpec(memory_space=pltpu.VMEM),) * 2,
        scratch_shapes=[
            vmem((rows, pix), BF16),
            vmem((1, rows), F32),
            vmem((1, rows), jnp.int32),
            vmem((1, rows), jnp.int32),
            vmem((n_hi, LANES), F32),
            vmem((1, n_cls), F32),
            vmem((n_block, n_pix, PANEL_DEV, rows // n_block), BF16),
            vmem((PANEL_DEV, rows), F32),
            vmem((rows, LANES), BF16),
            vmem((TILE if rows % (n_block * TILE) == 0 else rows // n_block, ch), BF16),
            vmem((max(n_panel + EXTRA, LANES), rows), BF16),
            vmem((8, pix), F32),
            vmem((n_panel + 8, pix), F32),
            vmem((half + 8, pix), F32),
            vmem((n_pix, PANEL_DEV, LANES), F32),
            vmem((half, LANES), F32),
            vmem((n_pix // 2, PANEL_DEV, LANES), F32),
            dma((n_block, pix // ch)),
            dma((6,)),
            dma((2,)),
            dma((n_block + 1, 2)),
            dma((1,)),
            dma((pix // ch + 2,)),
            dma((2,)),
        ],
        compiler_params=pltpu.CompilerParams(
            collective_id=0, has_side_effects=True, vmem_limit_bytes=60 * 1024 * 1024,
        ),
    )(
        response,
        vis_data.reshape(1, rows),
        baseline_of_row.reshape(1, rows),
        noise_class.reshape(1, rows),
        baseline_weight.reshape(n_hi, LANES),
        class_inv_var.reshape(1, n_cls),
    )
    sky, psf = pl.pallas_call(
        flush,
        out_shape=(
            jax.ShapeDtypeStruct((1, pix), F32),
            jax.ShapeDtypeStruct((half, pix), F32),
        ),
        in_specs=[pl.BlockSpec(memory_space=pltpu.VMEM)] * 2,
        out_specs=(pl.BlockSpec(memory_space=pltpu.HBM),) * 2,
        scratch_shapes=[dma((2,))],
    )(
        pltpu.with_memory_space_constraint(sky, pltpu.VMEM),
        pltpu.with_memory_space_constraint(psf, pltpu.VMEM),
    )
    return sky.reshape(pix), psf.T


def solution(mesh):
    placed = (P(("chan", "vis"), "pix"), P(("chan", "vis")), P("vis"), P("vis"), P(), P("chan"))
    return jax.shard_map(
        functools.partial(shards, mesh.shape["pix"]),
        mesh=mesh,
        in_specs=placed,
        out_specs=(P(("chan", "pix")), P(("chan", "pix"), "vis")),
        check_vma=False,
    )
```
